512 devices in a mesh: group: 2 (over y), blk: 32 (over z, core), uly: 8 (over x).
Axes of the slice: x: 8, y: 2, z: 16, core: 2. Of those that a mesh axis runs over, the one named last changes fastest.
The devices are a block of a 8x8x16 slice.
Arguments:
- query: bfloat16 [12288, 3072], P(('group', 'blk', 'uly')), parts along dimension 0, may hold values from -16 to 16
- keys: bfloat16 [12288, 3072], P(('group', 'blk', 'uly')), parts along dimension 0, may hold values from -16 to 16
- values: bfloat16 [12288, 3072], P(('group', 'blk', 'uly')), parts along dimension 0, may hold values from -6 to 6
- out_weight: bfloat16 [3072, 3072], P('uly', 'blk'), may hold values from -1 to 1
- out_gain: float32 [3072], replicated, may hold values from 0.1 to 1.9
Outputs:
- gated_out: bfloat16 [12288, 3072], P(('group', 'blk', 'uly')), parts along dimension 0
The draws below stay inside these ranges and needn't reach their ends.
There are 2 independent parts, one for each index of `group`. The reference program is written for one: setup_inputs(seed, part) draws one part's arguments, and reference() takes and returns one part's arrays. A program takes and returns all parts, laid end to end along the dimension named above; an argument that names none is the same for every part. Nothing has to cross between parts.
All inputs are finite; a program needn't handle non-finite values.
Results may differ from the reference program's by a relative error of at most 0.015.
Values may be sent and summed in bfloat16 or wider, within the bound.
No kernel may reach another device: no remote copies, remote signals or barrier semaphores. Data moves between devices by JAX's collectives and lax.ppermute only.
A program may use at most 128 MiB of HBM per device.

```python
import math
import jax
import jax.numpy as jnp
from jax import lax

D = 3072
H = 48
HEAD = 64
TOKENS = 6144


def pair_draw(key):
    key_query, key_keys = jax.random.split(jax.random.fold_in(key, 7013), 2)
    query = jnp.clip(1.4 * jax.random.normal(key_query, (TOKENS, D), jnp.float32), -8.0, 8.0)
    keys = jnp.clip(1.4 * jax.random.normal(key_keys, (TOKENS, D), jnp.float32), -8.0, 8.0)
    return (query, keys)


def draw_query(key, part):
    return pair_draw(key)[0].astype(jnp.bfloat16)


def draw_keys(key, part):
    return pair_draw(key)[1].astype(jnp.bfloat16)


def level_of(rng, shape, pieces, smallest, high):
    gain, own = 1.0, jax.random.fold_in(rng, 6)
    for axis_at, shards_of in pieces:
        heights = jnp.exp(jax.random.uniform(jax.random.fold_in(own, axis_at), (shards_of,), jnp.float32, smallest / len(pieces), high / len(pieces)))
        gain = gain * jnp.repeat(heights, shape[axis_at] // shards_of).reshape([-1 if axis == axis_at else 1 for axis in range(len(shape))])
    return gain


def scatter_about(key, shape, deviation, bound, cuts=(), held_as=jnp.bfloat16):
    drawn = jax.random.normal(key, shape, jnp.float32) * deviation
    if len(cuts) > 0:
        drawn = level_of(key, shape, cuts, -0.22, 0.18) * drawn
    return jnp.clip(drawn, min=-bound, max=bound).astype(held_as)


def setup_inputs(seed: int = 0, part: int = 0) -> dict:
    arg_keys = jax.random.split(jax.random.key(seed), 6)
    own_keys = jax.random.split(jax.random.fold_in(arg_keys[5], part), 6)
    query = draw_query(jax.random.fold_in(jax.random.fold_in(arg_keys[5], part), 71), part)
    keys = draw_keys(jax.random.fold_in(jax.random.fold_in(arg_keys[5], part), 71), part)
    values = scatter_about(own_keys[2], (TOKENS, D), 1.0, 6.0, ((0, 256),))
    out_weight = scatter_about(arg_keys[3], (D, D), (HEAD // 2) ** -0.5, 1.0, ((0, 8), (1, 32)))
    out_gain = jnp.clip(1.0 + 0.18 * jax.random.normal(arg_keys[4], (D,), jnp.float32), 0.1, 1.9)
    return {"query": query, "keys": keys, "values": values, "out_weight": out_weight, "out_gain": out_gain}


def reference(query, keys, values, out_weight, out_gain):
    score_scale = 1.0 / math.sqrt(HEAD)
    query_heads = query.reshape(TOKENS, H, HEAD).transpose(1, 0, 2)
    key_heads = keys.reshape(TOKENS, H, HEAD).transpose(1, 0, 2)
    value_heads = values.reshape(TOKENS, H, HEAD).transpose(1, 0, 2)

    def attend(triple):
        query_one, key_one, value_one = triple
        scores = jnp.dot(query_one, key_one.T, preferred_element_type=jnp.float32) * score_scale
        row_max = lax.optimization_barrier(jnp.max(scores, axis=1, keepdims=True))
        weights = jnp.exp(scores - row_max)
        denominator = lax.optimization_barrier(jnp.sum(weights, axis=1, keepdims=True))
        return jnp.dot(weights.astype(jnp.bfloat16), value_one, preferred_element_type=jnp.float32) / denominator
    per_head = lax.map(attend, (query_heads, key_heads, value_heads))
    attended = per_head.transpose(1, 0, 2).reshape(TOKENS, D).astype(jnp.bfloat16)
    projected = jnp.dot(attended, out_weight, preferred_element_type=jnp.float32)
    return (out_gain * projected).astype(jnp.bfloat16)
```

```python
import functools
import math

import jax
import jax.numpy as jnp
from jax import lax
from jax.experimental import pallas as pl
from jax.experimental.pallas import tpu as pltpu
from jax.sharding import PartitionSpec as P

HEAD = 64
PAIR = 2 * HEAD
LOG2E = math.log2(math.e)


def nt_dot(a, b):
    return lax.dot_general(a, b, (((1,), (1,)), ((), ())), preferred_element_type=jnp.float32)


def fold_kernel(first, q_ref, *refs):
    kv_refs = refs[:-3] if first else refs[:-6]
    new_max_ref, new_den_ref, new_sum_ref = refs[-3:]
    features = q_ref.shape[1]
    for pair in range(features // PAIR):
        cols = slice(pair * PAIR, (pair + 1) * PAIR)
        q_pair = q_ref[:, cols]
        lane = lax.broadcasted_iota(jnp.int32, q_pair.shape, 1)
        k_parts = [ref[:, cols] for ref in kv_refs]
        v_parts = [ref[:, slice(features + cols.start, features + cols.stop)].T for ref in kv_refs]
        for half in range(2):
            head = 2 * pair + half
            mine = (lane < HEAD) if half == 0 else (lane >= HEAD)
            q_head = jnp.where(mine, q_pair, jnp.zeros_like(q_pair))
            scores = [nt_dot(k, q_head) for k in k_parts]
            top = jnp.max(scores[0], axis=0, keepdims=True)
            for s in scores[1:]:
                top = jnp.maximum(top, jnp.max(s, axis=0, keepdims=True))
            if not first:
                old_max = refs[-6][head : head + 1, :]
                top = jnp.maximum(top, old_max)
                shrink = jnp.exp2((old_max - top) * LOG2E)
            den, acc = 0.0, 0.0
            for s, v in zip(scores, v_parts):
                weights = jnp.exp2((s - top) * LOG2E)
                den = den + jnp.sum(weights, axis=0, keepdims=True)
                acc = acc + jnp.dot(
                    v[half * HEAD : (half + 1) * HEAD, :],
                    weights.astype(jnp.bfloat16),
                    preferred_element_type=jnp.float32,
                )
            rows = slice(head * HEAD, (head + 1) * HEAD)
            if not first:
                den = den + refs[-5][head : head + 1, :] * shrink
                acc = acc + refs[-4][rows, :] * shrink
            new_max_ref[head : head + 1, :] = top
            new_den_ref[head : head + 1, :] = den
            new_sum_ref[rows, :] = acc


def fold(query_rows, blocks, state):
    row_count, features = query_rows.shape
    heads = features // HEAD
    vmem = pl.BlockSpec(memory_space=pltpu.VMEM)
    operands = (query_rows, *blocks, *(state or ()))
    key_count = sum(b.shape[0] for b in blocks)
    return pl.pallas_call(
        functools.partial(fold_kernel, state is None),
        out_shape=(
            jax.ShapeDtypeStruct((heads, row_count), jnp.float32),
            jax.ShapeDtypeStruct((heads, row_count), jnp.float32),
            jax.ShapeDtypeStruct((features, row_count), jnp.float32),
        ),
        in_specs=[vmem] * len(operands),
        out_specs=(vmem,) * 3,
        cost_estimate=pl.CostEstimate(
            flops=4 * row_count * key_count * features,
            bytes_accessed=2 * key_count * features * 2,
            transcendentals=row_count * key_count * heads,
        ),
    )(*operands)


def merge_kernel(m_ref, d_ref, s_ref, om_ref, od_ref, os_ref, out_ref):
    heads = m_ref.shape[0]
    top = jnp.maximum(m_ref[...], om_ref[...])
    mine = jnp.exp2((m_ref[...] - top) * LOG2E)
    theirs = jnp.exp2((om_ref[...] - top) * LOG2E)
    den = d_ref[...] * mine + od_ref[...] * theirs
    mine, theirs = mine / den, theirs / den
    for head in range(heads):
        rows = slice(head * HEAD, (head + 1) * HEAD)
        out_ref[rows, :] = (
            s_ref[rows, :] * mine[head : head + 1, :] + os_ref[rows, :] * theirs[head : head + 1, :]
        ).astype(out_ref.dtype)


def merge(state, other):
    features, row_count = state[2].shape
    vmem = pl.BlockSpec(memory_space=pltpu.VMEM)
    return pl.pallas_call(
        merge_kernel,
        out_shape=jax.ShapeDtypeStruct((features, row_count), jnp.bfloat16),
        in_specs=[vmem] * 6,
        out_specs=vmem,
    )(*state, *other)


def on_device(query, keys, values, out_weight, out_gain):
    tokens, width = query.shape
    blk, uly = lax.axis_size("blk"), lax.axis_size("uly")
    depth = blk // 2
    features = width // uly
    core = lax.axis_index("blk") % 2
    swap = [(i, i ^ 1) for i in range(blk)]
    ring = [
        (2 * z + c, 2 * ((z + (1 if c == 0 else -1)) % depth) + c)
        for z in range(depth)
        for c in range(2)
    ]

    cut = [a.reshape(tokens, uly, features) for a in (query * 0.125, keys, values)]
    packed = jnp.concatenate(cut, axis=2).transpose(1, 0, 2)
    own = lax.all_to_all(packed, "uly", 0, 0, tiled=True).reshape(tokens * uly, 3 * features)
    own_kv = own[:, features:]
    other = lax.ppermute(own, "blk", swap)
    other_kv = other[:, features:]
    rows = tokens * uly
    q_own, q_other = own[:, :features], other[:, :features]
    first_core = core == 0
    q_all = jnp.concatenate(
        [jnp.where(first_core, q_own, q_other), jnp.where(first_core, q_other, q_own)], axis=0
    )

    weight = lax.all_gather(out_weight, "blk", axis=1, tiled=True)

    state = fold(q_all, (own_kv,), None)
    a, b = own_kv, other_kv
    for step in range(1, depth // 2 + 1):
        a = lax.ppermute(a, "blk", ring)
        if step < depth // 2:
            b = lax.ppermute(b, "blk", ring)
            state = fold(q_all, (a, b), state)
        else:
            state = fold(q_all, (a,), state)
    theirs = [lax.ppermute(x, "blk", swap) for x in state]
    attended = merge(state, theirs)
    attended = lax.dynamic_slice_in_dim(attended, core * rows, rows, axis=1)
    partial = lax.dot_general(
        attended, weight, (((0,), (0,)), ((), ())), preferred_element_type=jnp.float32
    )
    blocks = lax.all_to_all(
        partial.astype(jnp.bfloat16).reshape(uly, tokens, width), "uly", 0, 0, tiled=True
    )
    summed = jnp.sum(blocks.astype(jnp.float32), axis=0)
    return (out_gain * summed).astype(jnp.bfloat16)


def solution(mesh):
    in_specs = (
        P(("group", "blk", "uly"), None),
        P(("group", "blk", "uly"), None),
        P(("group", "blk", "uly"), None),
        P("uly", "blk"),
        P(),
    )
    out_specs = P(("group", "blk", "uly"), None)
    return jax.shard_map(
        on_device, mesh=mesh, in_specs=in_specs, out_specs=out_specs, check_vma=False
    )
```

```python
import functools
import math

import jax
import jax.numpy as jnp
from jax import lax
from jax.experimental import pallas as pl
from jax.experimental.pallas import tpu as pltpu
from jax.sharding import PartitionSpec as P


HEAD = 64
PAIR = 2 * HEAD
STATS = 8
VMEM_LIMIT = 16 * 1024 * 1024
LOG2E = math.log2(math.e)


def nt_dot(a, b):
    return lax.dot_general(a, b, (((1,), (1,)), ((), ())), preferred_element_type=jnp.float32)


def fold_kernel(first, q_ref, *refs):
    state_ref, new_ref = (None, refs[-1]) if first else refs[-2:]
    kv_refs = refs[:-1] if first else refs[:-2]
    features = q_ref.shape[1]
    for pair in range(features // PAIR):
        cols = slice(pair * PAIR, (pair + 1) * PAIR)
        q_pair = q_ref[:, cols]
        lane = lax.broadcasted_iota(jnp.int32, q_pair.shape, 1)
        k_parts = [ref[:, cols] for ref in kv_refs]
        v_parts = [ref[:, slice(features + cols.start, features + cols.stop)].T for ref in kv_refs]
        for half in range(2):
            head = 2 * pair + half
            rows = slice(head * HEAD, (head + 1) * HEAD)
            max_row = slice(features + head, features + head + 1)
            den_row = slice(features + STATS + head, features + STATS + head + 1)
            mine = (lane < HEAD) if half == 0 else (lane >= HEAD)
            q_head = jnp.where(mine, q_pair, jnp.zeros_like(q_pair))
            scores = [nt_dot(k, q_head) for k in k_parts]
            top = jnp.max(scores[0], axis=0, keepdims=True)
            for s in scores[1:]:
                top = jnp.maximum(top, jnp.max(s, axis=0, keepdims=True))
            if not first:
                old_max = state_ref[max_row, :]
                top = jnp.maximum(top, old_max)
                shrink = jnp.exp2((old_max - top) * LOG2E)
            den, acc = 0.0, 0.0
            for s, v in zip(scores, v_parts):
                weights = jnp.exp2((s - top) * LOG2E)
                den = den + jnp.sum(weights, axis=0, keepdims=True)
                acc = acc + jnp.dot(
                    v[half * HEAD : (half + 1) * HEAD, :],
                    weights.astype(jnp.bfloat16),
                    preferred_element_type=jnp.float32,
                )
            if not first:
                den = den + state_ref[den_row, :] * shrink
                acc = acc + state_ref[rows, :] * shrink
            new_ref[max_row, :] = top
            new_ref[den_row, :] = den
            new_ref[rows, :] = acc


def fold(query_rows, blocks, state):
    row_count, features = query_rows.shape
    vmem = pl.BlockSpec(memory_space=pltpu.VMEM)
    operands = (query_rows, *blocks) if state is None else (query_rows, *blocks, state)
    key_count = sum(b.shape[0] for b in blocks)
    return pl.pallas_call(
        functools.partial(fold_kernel, state is None),
        out_shape=jax.ShapeDtypeStruct((features + 2 * STATS, row_count), jnp.float32),
        in_specs=[vmem] * len(operands),
        out_specs=vmem,
        compiler_params=pltpu.CompilerParams(vmem_limit_bytes=VMEM_LIMIT),
        cost_estimate=pl.CostEstimate(
            flops=4 * row_count * key_count * features,
            bytes_accessed=4 * key_count * features,
            transcendentals=row_count * key_count * (features // HEAD),
        ),
    )(*operands)


def merge_kernel(one_ref, two_ref, out_ref):
    features = out_ref.shape[1]
    heads = features // HEAD
    max_rows, den_rows = (slice(features + i, features + i + heads) for i in (0, STATS))
    one_max, two_max = one_ref[max_rows, :], two_ref[max_rows, :]
    top = jnp.maximum(one_max, two_max)
    one, two = (jnp.exp2((m - top) * LOG2E) for m in (one_max, two_max))
    den = one_ref[den_rows, :] * one + two_ref[den_rows, :] * two
    one, two = one / den, two / den
    parts = []
    for head in range(heads):
        rows, row = slice(head * HEAD, (head + 1) * HEAD), slice(head, head + 1)
        parts.append(one_ref[rows, :] * one[row, :] + two_ref[rows, :] * two[row, :])
    out_ref[...] = jnp.concatenate(parts, axis=0).astype(out_ref.dtype).T


def merge(one, two, features):
    vmem = pl.BlockSpec(memory_space=pltpu.VMEM)
    return pl.pallas_call(
        merge_kernel,
        out_shape=jax.ShapeDtypeStruct((one.shape[1], features), jnp.bfloat16),
        in_specs=[vmem] * 2,
        out_specs=vmem,
        compiler_params=pltpu.CompilerParams(vmem_limit_bytes=VMEM_LIMIT),
    )(one, two)


def on_device(query, keys, values, out_weight, out_gain):
    tokens, width = query.shape
    blk, uly = lax.axis_size("blk"), lax.axis_size("uly")
    depth, quad = blk // 2, uly // 2
    features = width // uly
    rows = tokens * uly
    core = lax.axis_index("blk") % 2
    side = lax.axis_index("uly") // quad
    swap = [(i, i ^ 1) for i in range(blk)]
    ring = [
        (2 * z + c, 2 * ((z + (1 if c == 0 else -1)) % depth) + c)
        for z in range(depth)
        for c in range(2)
    ]
    across = [(i, (i + quad) % uly) for i in range(uly)]
    quads = [[h * quad + i for i in range(quad)] for h in range(2)]

    far_weight = lax.ppermute(out_weight, "uly", across)
    both = jnp.concatenate([out_weight, far_weight], axis=0)
    weight = lax.all_gather(both, "blk", axis=1, tiled=True)

    cut = [a.reshape(tokens, uly, features) for a in (query, keys, values)]
    packed = jnp.concatenate(cut, axis=2).transpose(1, 0, 2)
    own = lax.all_to_all(packed, "uly", 0, 0, tiled=True).reshape(rows, 3 * features)
    other = lax.ppermute(own, "blk", swap)
    q_own, q_other = own[:, :features], other[:, :features]
    q_all = jnp.concatenate(
        [jnp.where(core == 0, q_own, q_other), jnp.where(core == 0, q_other, q_own)], axis=0
    ) * jnp.bfloat16(1.0 / math.sqrt(HEAD))

    a, b = own[:, features:], other[:, features:]
    state = fold(q_all, (a,), None)
    last = depth // 2
    for step in range(1, last + 1):
        a = lax.ppermute(a, "blk", ring)
        if step < last:
            b = lax.ppermute(b, "blk", ring)
        state = fold(q_all, (a, b) if step < last else (a,), state)
    theirs = lax.ppermute(state, "blk", swap)
    attended = merge(state, theirs, features)

    half = quad * tokens
    near = lax.dynamic_slice_in_dim(attended, core * rows + side * half, half, axis=0)
    far = lax.dynamic_slice_in_dim(attended, core * rows + (1 - side) * half, half, axis=0)
    far = lax.ppermute(far, "uly", across)
    joined = jnp.concatenate([near, far], axis=1)
    partial = jnp.dot(joined, weight, preferred_element_type=jnp.float32).astype(jnp.bfloat16)
    blocks = lax.all_to_all(
        partial.reshape(quad, tokens, width), "uly", 0, 0, tiled=True, axis_index_groups=quads
    )
    summed = jnp.sum(blocks.astype(jnp.float32), axis=0)
    return (out_gain * summed).astype(jnp.bfloat16)


def solution(mesh):
    in_specs = (
        P(("group", "blk", "uly"), None),
        P(("group", "blk", "uly"), None),
        P(("group", "blk", "uly"), None),
        P("uly", "blk"),
        P(),
    )
    out_specs = P(("group", "blk", "uly"), None)
    return jax.shard_map(
        on_device, mesh=mesh, in_specs=in_specs, out_specs=out_specs, check_vma=False
    )
```

```python
import functools
import math

import jax
import jax.numpy as jnp
from jax import lax
from jax.experimental import pallas as pl
from jax.experimental.pallas import tpu as pltpu
from jax.sharding import PartitionSpec as P


HEAD = 64
PAIR = 2 * HEAD
STATS = 8
VMEM_LIMIT = 16 * 1024 * 1024
LOG2E = math.log2(math.e)


def nt_dot(a, b):
    return lax.dot_general(a, b, (((1,), (1,)), ((), ())), preferred_element_type=jnp.float32)


def fold_kernel(first, q_ref, *refs):
    state_ref, new_ref = (None, refs[-1]) if first else refs[-2:]
    kv_refs = refs[:-1] if first else refs[:-2]
    features = q_ref.shape[1]
    for pair in range(features // PAIR):
        cols = slice(pair * PAIR, (pair + 1) * PAIR)
        q_pair = q_ref[:, cols]
        lane = lax.broadcasted_iota(jnp.int32, q_pair.shape, 1)
        k_parts = [ref[:, cols] for ref in kv_refs]
        v_parts = [ref[:, slice(features + cols.start, features + cols.stop)].T for ref in kv_refs]
        for half in range(2):
            head = 2 * pair + half
            rows = slice(head * HEAD, (head + 1) * HEAD)
            max_row = slice(features + head, features + head + 1)
            den_row = slice(features + STATS + head, features + STATS + head + 1)
            mine = (lane < HEAD) if half == 0 else (lane >= HEAD)
            q_head = jnp.where(mine, q_pair, jnp.zeros_like(q_pair))
            scores = [nt_dot(k, q_head) for k in k_parts]
            top = jnp.max(scores[0], axis=0, keepdims=True)
            for s in scores[1:]:
                top = jnp.maximum(top, jnp.max(s, axis=0, keepdims=True))
            if not first:
                old_max = state_ref[max_row, :]
                top = jnp.maximum(top, old_max)
                shrink = jnp.exp2((old_max - top) * LOG2E)
            den, acc = 0.0, 0.0
            for s, v in zip(scores, v_parts):
                weights = jnp.exp2((s - top) * LOG2E)
                den = den + jnp.sum(weights, axis=0, keepdims=True)
                acc = acc + jnp.dot(
                    v[half * HEAD : (half + 1) * HEAD, :],
                    weights.astype(jnp.bfloat16),
                    preferred_element_type=jnp.float32,
                )
            if not first:
                den = den + state_ref[den_row, :] * shrink
                acc = acc + state_ref[rows, :] * shrink
            new_ref[max_row, :] = top
            new_ref[den_row, :] = den
            new_ref[rows, :] = acc


def fold(query_rows, blocks, state):
    row_count, features = query_rows.shape
    vmem = pl.BlockSpec(memory_space=pltpu.VMEM)
    operands = (query_rows, *blocks) if state is None else (query_rows, *blocks, state)
    key_count = sum(b.shape[0] for b in blocks)
    return pl.pallas_call(
        functools.partial(fold_kernel, state is None),
        out_shape=jax.ShapeDtypeStruct((features + 2 * STATS, row_count), jnp.float32),
        in_specs=[vmem] * len(operands),
        out_specs=vmem,
        compiler_params=pltpu.CompilerParams(vmem_limit_bytes=VMEM_LIMIT),
        cost_estimate=pl.CostEstimate(
            flops=4 * row_count * key_count * features,
            bytes_accessed=4 * key_count * features,
            transcendentals=row_count * key_count * (features // HEAD),
        ),
    )(*operands)


def merged(one_ref, two_ref, features):
    heads = features // HEAD
    max_rows, den_rows = (slice(features + i, features + i + heads) for i in (0, STATS))
    one_max, two_max = one_ref[max_rows, :], two_ref[max_rows, :]
    top = jnp.maximum(one_max, two_max)
    one, two = (jnp.exp2((m - top) * LOG2E) for m in (one_max, two_max))
    den = one_ref[den_rows, :] * one + two_ref[den_rows, :] * two
    one, two = one / den, two / den
    parts = []
    for head in range(heads):
        rows, row = slice(head * HEAD, (head + 1) * HEAD), slice(head, head + 1)
        parts.append(one_ref[rows, :] * one[row, :] + two_ref[rows, :] * two[row, :])
    return jnp.concatenate(parts, axis=0).astype(jnp.bfloat16).T


def project_kernel(
    depth, place_ref, one_ref, two_ref, self_ref, mine_ref, theirs_ref, out_ref, attended, weight
):
    z, core = place_ref[0], place_ref[1]
    rows, width = out_ref.shape
    features = attended.shape[1]
    pair = self_ref.shape[0]
    cols = pair // 2
    last = depth // 2

    def put(chip, offset, block):
        at = pl.multiple_of(lax.rem(chip, depth) * pair + offset, 16)
        weight[pl.ds(at, block.shape[0]), :] = block

    put(z, 0, self_ref[...])
    for step in range(1, last):
        block = slice((step - 1) * pair, step * pair)
        ahead, behind = z + step, z + depth - step
        put(jnp.where(core == 0, ahead, behind), 0, mine_ref[block, :])
        put(jnp.where(core == 0, behind, ahead), 0, theirs_ref[block, :])
    block = slice((last - 1) * pair, (last - 1) * pair + cols)
    put(z + last, core * cols, mine_ref[block, :])
    put(z + last, (1 - core) * cols, theirs_ref[block, :])

    attended[...] = merged(one_ref, two_ref, features)
    mine = attended[pl.ds(pl.multiple_of(core * rows, 16), rows), :]
    chunk = width // 4
    for i in range(4):
        part = slice(i * chunk, (i + 1) * chunk)
        out_ref[:, part] = nt_dot(mine, weight[part, :]).astype(out_ref.dtype)


def project(depth, place, one, two, weights):
    row_count = one.shape[1]
    features = weights[0].shape[1]
    width = weights[0].shape[0] * depth
    vmem = pl.BlockSpec(memory_space=pltpu.VMEM)
    return pl.pallas_call(
        functools.partial(project_kernel, depth),
        out_shape=jax.ShapeDtypeStruct((row_count // 2, width), jnp.bfloat16),
        in_specs=[pl.BlockSpec(memory_space=pltpu.SMEM)] + [vmem] * 5,
        out_specs=vmem,
        scratch_shapes=[
            pltpu.VMEM((row_count, features), jnp.bfloat16),
            pltpu.VMEM((width, features), jnp.bfloat16),
        ],
        compiler_params=pltpu.CompilerParams(vmem_limit_bytes=VMEM_LIMIT),
    )(place, one, two, *weights)


def on_device(query, keys, values, out_weight, out_gain):
    tokens, width = query.shape
    blk, uly = lax.axis_size("blk"), lax.axis_size("uly")
    depth = blk // 2
    last = depth // 2
    features = width // uly
    rows = tokens * uly
    z, core = lax.axis_index("blk") // 2, lax.axis_index("blk") % 2
    swap = [(i, i ^ 1) for i in range(blk)]
    ring, against = (
        [
            (2 * z + c, 2 * ((z + (way if c == 0 else -way)) % depth) + c)
            for z in range(depth)
            for c in range(2)
        ]
        for way in (1, -1)
    )

    def by_core(own, other):
        return jnp.concatenate(
            [jnp.where(core == 0, own, other), jnp.where(core == 0, other, own)], axis=0
        )

    columns = out_weight.T
    w_self = by_core(columns, lax.ppermute(columns, "blk", swap))

    cut = [a.reshape(tokens, uly, features) for a in (query, keys, values)]
    packed = jnp.concatenate(cut, axis=2).transpose(1, 0, 2)
    own = lax.all_to_all(packed, "uly", 0, 0, tiled=True).reshape(rows, 3 * features)
    other = lax.ppermute(own, "blk", swap)
    q_all = by_core(own[:, :features], other[:, :features])
    q_all = q_all * jnp.bfloat16(1.0 / math.sqrt(HEAD))

    a, b, w = own[:, features:], other[:, features:], w_self
    w_blocks = []
    state = fold(q_all, (a,), None)
    for step in range(1, last + 1):
        a = lax.ppermute(a, "blk", ring)
        if step < last:
            b = lax.ppermute(b, "blk", ring)
        else:
            half = w.shape[0] // 2
            w = lax.dynamic_slice_in_dim(w, core * half, half, axis=0)
        w = lax.ppermute(w, "blk", against)
        w_blocks.append(w)
        state = fold(q_all, (a, b) if step < last else (a,), state)
    w_mine = jnp.concatenate(w_blocks, axis=0)
    w_theirs = lax.ppermute(w_mine, "blk", swap)
    theirs = lax.ppermute(state, "blk", swap)
    place = jnp.stack([z, core]).astype(jnp.int32)
    partial = project(depth, place, state, theirs, (w_self, w_mine, w_theirs))
    blocks = lax.all_to_all(partial.reshape(uly, tokens, width), "uly", 0, 0, tiled=True)
    summed = jnp.sum(blocks.astype(jnp.float32), axis=0)
    return (out_gain * summed).astype(jnp.bfloat16)


def solution(mesh):
    in_specs = (
        P(("group", "blk", "uly"), None),
        P(("group", "blk", "uly"), None),
        P(("group", "blk", "uly"), None),
        P("uly", "blk"),
        P(),
    )
    out_specs = P(("group", "blk", "uly"), None)
    return jax.shard_map(
        on_device, mesh=mesh, in_specs=in_specs, out_specs=out_specs, check_vma=False
    )
```

```python
import functools
import math

import jax
import jax.numpy as jnp
from jax import lax
from jax.experimental import pallas as pl
from jax.experimental.pallas import tpu as pltpu
from jax.sharding import PartitionSpec as P


HEAD = 64
PAIR = 2 * HEAD
STATS = 8
VMEM_LIMIT = 16 * 1024 * 1024
LOG2E = math.log2(math.e)


def nt_dot(a, b):
    return lax.dot_general(a, b, (((1,), (1,)), ((), ())), preferred_element_type=jnp.float32)


def fold_kernel(first, q_ref, *refs):
    state_ref, new_ref = (None, refs[-1]) if first else refs[-2:]
    kv_refs = refs[:-1] if first else refs[:-2]
    features = q_ref.shape[1]
    for pair in range(features // PAIR):
        cols = slice(pair * PAIR, (pair + 1) * PAIR)
        q_pair = q_ref[:, cols]
        lane = lax.broadcasted_iota(jnp.int32, q_pair.shape, 1)
        k_parts = [ref[:, cols] for ref in kv_refs]
        v_parts = [ref[:, slice(features + cols.start, features + cols.stop)].T for ref in kv_refs]
        for half in range(2):
            head = 2 * pair + half
            rows = slice(head * HEAD, (head + 1) * HEAD)
            max_row = slice(features + head, features + head + 1)
            den_row = slice(features + STATS + head, features + STATS + head + 1)
            mine = (lane < HEAD) if half == 0 else (lane >= HEAD)
            q_head = jnp.where(mine, q_pair, jnp.zeros_like(q_pair))
            scores = [nt_dot(k, q_head) for k in k_parts]
            top = jnp.max(scores[0], axis=0, keepdims=True)
            for s in scores[1:]:
                top = jnp.maximum(top, jnp.max(s, axis=0, keepdims=True))
            if not first:
                old_max = state_ref[max_row, :]
                top = jnp.maximum(top, old_max)
                shrink = jnp.exp2((old_max - top) * LOG2E)
            den, acc = 0.0, 0.0
            for s, v in zip(scores, v_parts):
                weights = jnp.exp2((s - top) * LOG2E)
                den = den + jnp.sum(weights, axis=0, keepdims=True)
                acc = acc + jnp.dot(
                    v[half * HEAD : (half + 1) * HEAD, :],
                    weights.astype(jnp.bfloat16),
                    preferred_element_type=jnp.float32,
                )
            if not first:
                den = den + state_ref[den_row, :] * shrink
                acc = acc + state_ref[rows, :] * shrink
            new_ref[max_row, :] = top
            new_ref[den_row, :] = den
            new_ref[rows, :] = acc


def fold(query_rows, blocks, state):
    row_count, features = query_rows.shape
    vmem = pl.BlockSpec(memory_space=pltpu.VMEM)
    operands = (query_rows, *blocks) if state is None else (query_rows, *blocks, state)
    key_count = sum(b.shape[0] for b in blocks)
    return pl.pallas_call(
        functools.partial(fold_kernel, state is None),
        out_shape=jax.ShapeDtypeStruct((features + 2 * STATS, row_count), jnp.float32),
        in_specs=[vmem] * len(operands),
        out_specs=vmem,
        compiler_params=pltpu.CompilerParams(vmem_limit_bytes=VMEM_LIMIT),
        cost_estimate=pl.CostEstimate(
            flops=4 * row_count * key_count * features,
            bytes_accessed=4 * key_count * features,
            transcendentals=row_count * key_count * (features // HEAD),
        ),
    )(*operands)


def merged(one_ref, two_ref, features):
    heads = features // HEAD
    max_rows, den_rows = (slice(features + i, features + i + heads) for i in (0, STATS))
    one_max, two_max = one_ref[max_rows, :], two_ref[max_rows, :]
    top = jnp.maximum(one_max, two_max)
    one, two = (jnp.exp2((m - top) * LOG2E) for m in (one_max, two_max))
    den = one_ref[den_rows, :] * one + two_ref[den_rows, :] * two
    one, two = one / den, two / den
    parts = []
    for head in range(heads):
        rows, row = slice(head * HEAD, (head + 1) * HEAD), slice(head, head + 1)
        parts.append(one_ref[rows, :] * one[row, :] + two_ref[rows, :] * two[row, :])
    return jnp.concatenate(parts, axis=0).astype(jnp.bfloat16).T


def project_kernel(
    depth, place_ref, one_ref, two_ref, self_ref, mine_ref, theirs_ref, far_ref, out_ref, attended, weight
):
    z, core = place_ref[0], place_ref[1]
    rows, width = out_ref.shape
    features = attended.shape[1]
    pair = self_ref.shape[0]
    last = depth // 2

    def put(chip, block):
        at = pl.multiple_of(lax.rem(chip, depth) * pair, 16)
        weight[pl.ds(at, pair), :] = block

    put(z, self_ref[...])
    put(z + last, far_ref[...])
    for step in range(1, last):
        block = slice((step - 1) * pair, step * pair)
        ahead, behind = z + step, z + depth - step
        put(jnp.where(core == 0, ahead, behind), mine_ref[block, :])
        put(jnp.where(core == 0, behind, ahead), theirs_ref[block, :])

    attended[...] = merged(one_ref, two_ref, features)
    mine = attended[pl.ds(pl.multiple_of(core * rows, 16), rows), :]
    chunk = width // 4
    for i in range(4):
        part = slice(i * chunk, (i + 1) * chunk)
        out_ref[:, part] = nt_dot(mine, weight[part, :]).astype(out_ref.dtype)


def project(depth, place, one, two, weights):
    row_count = one.shape[1]
    features = weights[0].shape[1]
    width = weights[0].shape[0] * depth
    vmem = pl.BlockSpec(memory_space=pltpu.VMEM)
    return pl.pallas_call(
        functools.partial(project_kernel, depth),
        out_shape=jax.ShapeDtypeStruct((row_count // 2, width), jnp.bfloat16),
        in_specs=[pl.BlockSpec(memory_space=pltpu.SMEM)] + [vmem] * 6,
        out_specs=vmem,
        scratch_shapes=[
            pltpu.VMEM((row_count, features), jnp.bfloat16),
            pltpu.VMEM((width, features), jnp.bfloat16),
        ],
        compiler_params=pltpu.CompilerParams(vmem_limit_bytes=VMEM_LIMIT),
    )(place, one, two, *weights)


def weight_hops(depth):
    held, hops, last = 1, [], depth // 2
    while held <= last:
        hops.append(min(held, 3, last + 1 - held))
        held += hops[-1]
    return hops


def on_device(query, keys, values, out_weight, out_gain):
    tokens, width = query.shape
    blk, uly = lax.axis_size("blk"), lax.axis_size("uly")
    depth = blk // 2
    last = depth // 2
    features = width // uly
    rows = tokens * uly
    z, core = lax.axis_index("blk") // 2, lax.axis_index("blk") % 2
    swap = [(i, i ^ 1) for i in range(blk)]

    def round_z(hop):
        return [
            (2 * z + c, 2 * ((z + (hop if c == 0 else -hop)) % depth) + c)
            for z in range(depth)
            for c in range(2)
        ]

    ring = round_z(1)

    def by_core(own, other):
        return jnp.concatenate(
            [jnp.where(core == 0, own, other), jnp.where(core == 0, other, own)], axis=0
        )

    columns = out_weight.T
    w_self = by_core(columns, lax.ppermute(columns, "blk", swap))

    cut = [a.reshape(tokens, uly, features) for a in (query, keys, values)]
    packed = jnp.concatenate(cut, axis=2).transpose(1, 0, 2)
    own = lax.all_to_all(packed, "uly", 0, 0, tiled=True).reshape(rows, 3 * features)
    other = lax.ppermute(own, "blk", swap)
    q_all = by_core(own[:, :features], other[:, :features])
    q_all = q_all * jnp.bfloat16(1.0 / math.sqrt(HEAD))

    pair = w_self.shape[0]
    held, w_parts = 1, [w_self]
    for hop in weight_hops(depth):
        send = jnp.concatenate(w_parts, axis=0)[(held - hop) * pair :]
        w_parts.append(lax.ppermute(send, "blk", round_z(-hop)))
        held += hop
    w_got = jnp.concatenate(w_parts[1:], axis=0)
    w_mine, w_far = w_got[:-pair], w_got[-pair:]
    w_theirs = lax.ppermute(w_mine, "blk", swap)

    a, b = own[:, features:], other[:, features:]
    state = fold(q_all, (a,), None)
    for step in range(1, last + 1):
        a = lax.ppermute(a, "blk", ring)
        if step < last:
            b = lax.ppermute(b, "blk", ring)
        state = fold(q_all, (a, b) if step < last else (a,), state)
    theirs = lax.ppermute(state, "blk", swap)
    place = jnp.stack([z, core]).astype(jnp.int32)
    partial = project(depth, place, state, theirs, (w_self, w_mine, w_theirs, w_far))
    blocks = lax.all_to_all(partial.reshape(uly, tokens, width), "uly", 0, 0, tiled=True)
    summed = jnp.sum(blocks.astype(jnp.float32), axis=0)
    return (out_gain * summed).astype(jnp.bfloat16)


def solution(mesh):
    in_specs = (
        P(("group", "blk", "uly"), None),
        P(("group", "blk", "uly"), None),
        P(("group", "blk", "uly"), None),
        P("uly", "blk"),
        P(),
    )
    out_specs = P(("group", "blk", "uly"), None)
    return jax.shard_map(
        on_device, mesh=mesh, in_specs=in_specs, out_specs=out_specs, check_vma=False
    )
```

```python
import functools
import math

import jax
import jax.numpy as jnp
from jax import lax
from jax.experimental import pallas as pl
from jax.experimental.pallas import tpu as pltpu
from jax.sharding import PartitionSpec as P


HEAD = 64
PAIR = 2 * HEAD
STATS = 8
VMEM_LIMIT = 16 * 1024 * 1024
LOG2E = math.log2(math.e)


def nt_dot(a, b):
    return lax.dot_general(a, b, (((1,), (1,)), ((), ())), preferred_element_type=jnp.float32)


def fold_kernel(first, q_ref, *refs):
    state_ref, new_ref = (None, refs[-1]) if first else refs[-2:]
    kv_refs = refs[:-1] if first else refs[:-2]
    features = q_ref.shape[1]
    for pair in range(features // PAIR):
        cols = slice(pair * PAIR, (pair + 1) * PAIR)
        q_pair = q_ref[:, cols]
        lane = lax.broadcasted_iota(jnp.int32, q_pair.shape, 1)
        k_parts = [ref[:, cols] for ref in kv_refs]
        v_parts = [ref[:, slice(features + cols.start, features + cols.stop)].T for ref in kv_refs]
        for half in range(2):
            head = 2 * pair + half
            rows = slice(head * HEAD, (head + 1) * HEAD)
            max_row = slice(features + head, features + head + 1)
            den_row = slice(features + STATS + head, features + STATS + head + 1)
            mine = (lane < HEAD) if half == 0 else (lane >= HEAD)
            q_head = jnp.where(mine, q_pair, jnp.zeros_like(q_pair))
            scores = [nt_dot(k, q_head) for k in k_parts]
            top = jnp.max(scores[0], axis=0, keepdims=True)
            for s in scores[1:]:
                top = jnp.maximum(top, jnp.max(s, axis=0, keepdims=True))
            if not first:
                old_max = state_ref[max_row, :]
                top = jnp.maximum(top, old_max)
                shrink = jnp.exp2((old_max - top) * LOG2E)
            den, acc = 0.0, 0.0
            for s, v in zip(scores, v_parts):
                weights = jnp.exp2((s - top) * LOG2E)
                den = den + jnp.sum(weights, axis=0, keepdims=True)
                acc = acc + jnp.dot(
                    v[half * HEAD : (half + 1) * HEAD, :],
                    weights.astype(jnp.bfloat16),
                    preferred_element_type=jnp.float32,
                )
            if not first:
                den = den + state_ref[den_row, :] * shrink
                acc = acc + state_ref[rows, :] * shrink
            new_ref[max_row, :] = top
            new_ref[den_row, :] = den
            new_ref[rows, :] = acc


def fold(query_rows, blocks, state):
    row_count, features = query_rows.shape
    vmem = pl.BlockSpec(memory_space=pltpu.VMEM)
    operands = (query_rows, *blocks) if state is None else (query_rows, *blocks, state)
    key_count = sum(b.shape[0] for b in blocks)
    return pl.pallas_call(
        functools.partial(fold_kernel, state is None),
        out_shape=jax.ShapeDtypeStruct((features + 2 * STATS, row_count), jnp.float32),
        in_specs=[vmem] * len(operands),
        out_specs=vmem,
        compiler_params=pltpu.CompilerParams(vmem_limit_bytes=VMEM_LIMIT),
        cost_estimate=pl.CostEstimate(
            flops=4 * row_count * key_count * features,
            bytes_accessed=4 * key_count * features,
            transcendentals=row_count * key_count * (features // HEAD),
        ),
    )(*operands)


def merged(one_ref, two_ref, features):
    heads = features // HEAD
    max_rows, den_rows = (slice(features + i, features + i + heads) for i in (0, STATS))
    one_max, two_max = one_ref[max_rows, :], two_ref[max_rows, :]
    top = jnp.maximum(one_max, two_max)
    one, two = (jnp.exp2((m - top) * LOG2E) for m in (one_max, two_max))
    den = one_ref[den_rows, :] * one + two_ref[den_rows, :] * two
    one, two = one / den, two / den
    parts = []
    for head in range(heads):
        rows, row = slice(head * HEAD, (head + 1) * HEAD), slice(head, head + 1)
        parts.append(one_ref[rows, :] * one[row, :] + two_ref[rows, :] * two[row, :])
    return jnp.concatenate(parts, axis=0).astype(jnp.bfloat16).T


def lay_out(weight, blocks, core, mine_ref, theirs_ref):
    pair = weight.shape[0] // (2 * len(blocks) + 1)
    for here, step in enumerate(blocks):
        block = slice(here * pair, (here + 1) * pair)
        for ref, way in ((mine_ref, 1 - 2 * core), (theirs_ref, 2 * core - 1)):
            at = pl.multiple_of((len(blocks) + way * step) * pair, 8)
            weight[pl.ds(at, pair), :] = ref[block, :]


def times_weight(mine, weight, out_ref):
    chunks = 3
    chunk = weight.shape[0] // chunks if weight.shape[0] % (chunks * 128) == 0 else weight.shape[0]
    for at in range(0, weight.shape[0], chunk):
        part = slice(at, at + chunk)
        out_ref[:, part] = nt_dot(mine, weight[part, :]).astype(out_ref.dtype)


def near_kernel(
    core_ref, one_ref, two_ref, self_ref, mine_ref, theirs_ref, out_ref, own_ref, attended, weight
):
    core = core_ref[0]
    rows, features = own_ref.shape
    pair = self_ref.shape[0]
    near = mine_ref.shape[0] // pair
    weight[near * pair : (near + 1) * pair, :] = self_ref[...]
    lay_out(weight, range(1, near + 1), core, mine_ref, theirs_ref)
    attended[...] = merged(one_ref, two_ref, features)
    own_ref[...] = attended[pl.ds(pl.multiple_of(core * rows, 8), rows), :]
    times_weight(own_ref[...], weight, out_ref)


def far_kernel(core_ref, own_ref, mine_ref, theirs_ref, out_ref, weight):
    core = core_ref[0]
    pair = mine_ref.shape[0] - theirs_ref.shape[0]
    far = theirs_ref.shape[0] // pair
    weight[far * pair : (far + 1) * pair, :] = mine_ref[far * pair :, :]
    lay_out(weight, [i - far for i in range(far)], core, mine_ref, theirs_ref)
    times_weight(own_ref[...], weight, out_ref)


def project(kernel, core, operands, width, attended_shape=None):
    rows, features = attended_shape or operands[0].shape
    vmem = pl.BlockSpec(memory_space=pltpu.VMEM)
    out = jax.ShapeDtypeStruct((rows, width), jnp.bfloat16)
    weight = pltpu.VMEM((width, features), jnp.bfloat16)
    first = attended_shape is not None
    return pl.pallas_call(
        kernel,
        out_shape=(out, jax.ShapeDtypeStruct((rows, features), jnp.bfloat16)) if first else out,
        in_specs=[pl.BlockSpec(memory_space=pltpu.SMEM)] + [vmem] * len(operands),
        out_specs=(vmem, vmem) if first else vmem,
        scratch_shapes=(
            [pltpu.VMEM((2 * rows, features), jnp.bfloat16), weight] if first else [weight]
        ),
        compiler_params=pltpu.CompilerParams(vmem_limit_bytes=VMEM_LIMIT),
        cost_estimate=pl.CostEstimate(
            flops=2 * rows * features * width, bytes_accessed=2 * width * features, transcendentals=0
        ),
    )(core[None], *operands)


def weight_hops(depth):
    held, hops, last = 1, [], depth // 2
    while held <= last:
        hops.append(min(held, 3, last + 1 - held))
        held += hops[-1]
    return hops


EARLY = 2


def on_device(query, keys, values, out_weight, out_gain):
    tokens, width = query.shape
    blk, uly = lax.axis_size("blk"), lax.axis_size("uly")
    depth = blk // 2
    last = depth // 2
    features = width // uly
    rows = tokens * uly
    at = lax.axis_index("blk").astype(jnp.int32)
    z, core = lax.div(at, 2), lax.rem(at, 2)
    swap = [(i, i ^ 1) for i in range(blk)]

    def round_z(hop):
        return [
            (2 * z + c, 2 * ((z + (hop if c == 0 else -hop)) % depth) + c)
            for z in range(depth)
            for c in range(2)
        ]

    ring = round_z(1)

    def by_core(own, other):
        return jnp.concatenate(
            [jnp.where(core == 0, own, other), jnp.where(core == 0, other, own)], axis=0
        )

    columns = out_weight.T
    w_self = by_core(columns, lax.ppermute(columns, "blk", swap))

    cut = [a.reshape(tokens, uly, features) for a in (query, keys, values)]
    packed = jnp.concatenate(cut, axis=2).transpose(1, 0, 2)
    own = lax.all_to_all(packed, "uly", 0, 0, tiled=True).reshape(rows, 3 * features)
    other = lax.ppermute(own, "blk", swap)
    q_all = by_core(own[:, :features], other[:, :features])
    q_all = q_all * jnp.bfloat16(1.0 / math.sqrt(HEAD))

    pair = w_self.shape[0]
    hops = weight_hops(depth)
    held, w_parts = 1, [w_self]
    for hop in hops:
        send = jnp.concatenate(w_parts, axis=0)[(held - hop) * pair :]
        w_parts.append(lax.ppermute(send, "blk", round_z(-hop)))
        held += hop
    near = sum(hops[:EARLY])
    w_near, w_far = (
        jnp.concatenate(parts, axis=0) for parts in (w_parts[1 : EARLY + 1], w_parts[EARLY + 1 :])
    )
    near_theirs = lax.ppermute(w_near, "blk", swap)
    far_theirs = lax.ppermute(w_far[:-pair], "blk", swap)

    a, b = own[:, features:], other[:, features:]
    state = fold(q_all, (a,), None)
    for step in range(1, last + 1):
        a = lax.ppermute(a, "blk", ring)
        if step < last:
            b = lax.ppermute(b, "blk", ring)
        state = fold(q_all, (a, b) if step < last else (a,), state)
    theirs = lax.ppermute(state, "blk", swap)

    def exchanged(partial):
        blocks = partial.reshape(uly, tokens, partial.shape[1])
        blocks = lax.all_to_all(blocks, "uly", 0, 0, tiled=True)
        return jnp.sum(blocks.astype(jnp.float32), axis=0)

    near_width = (2 * near + 1) * pair
    partial, attended = project(
        near_kernel,
        core,
        (state, theirs, w_self, w_near, near_theirs),
        near_width,
        (rows, features),
    )
    near_sum = exchanged(partial)
    partial = project(far_kernel, core, (attended, w_far, far_theirs), width - near_width)
    far_sum = exchanged(partial)
    turned = jnp.concatenate([near_sum, far_sum] * 2, axis=1)
    summed = lax.dynamic_slice_in_dim(turned, lax.rem(near + depth - z, depth) * pair, width, axis=1)
    return (out_gain * summed).astype(jnp.bfloat16)


def solution(mesh):
    in_specs = (
        P(("group", "blk", "uly"), None),
        P(("group", "blk", "uly"), None),
        P(("group", "blk", "uly"), None),
        P("uly", "blk"),
        P(),
    )
    out_specs = P(("group", "blk", "uly"), None)
    return jax.shard_map(
        on_device, mesh=mesh, in_specs=in_specs, out_specs=out_specs, check_vma=False
    )
```

```python
import functools
import math

import jax
import jax.numpy as jnp
from jax import lax
from jax.experimental import pallas as pl
from jax.experimental.pallas import tpu as pltpu
from jax.sharding import PartitionSpec as P


HEAD = 64
PAIR = 2 * HEAD
STATS = 8
VMEM_LIMIT = 16 * 1024 * 1024
LOG2E = math.log2(math.e)


def nt_dot(a, b):
    return lax.dot_general(a, b, (((1,), (1,)), ((), ())), preferred_element_type=jnp.float32)


def fold_kernel(first, q_ref, *refs):
    state_ref, new_ref = (None, refs[-1]) if first else refs[-2:]
    kv_refs = refs[:-1] if first else refs[:-2]
    features = q_ref.shape[1]
    for pair in range(features // PAIR):
        cols = slice(pair * PAIR, (pair + 1) * PAIR)
        q_pair = q_ref[:, cols]
        lane = lax.broadcasted_iota(jnp.int32, q_pair.shape, 1)
        k_parts = [ref[:, cols] for ref in kv_refs]
        v_parts = [ref[:, slice(features + cols.start, features + cols.stop)].T for ref in kv_refs]
        for half in range(2):
            head = 2 * pair + half
            rows = slice(head * HEAD, (head + 1) * HEAD)
            max_row = slice(features + head, features + head + 1)
            den_row = slice(features + STATS + head, features + STATS + head + 1)
            mine = (lane < HEAD) if half == 0 else (lane >= HEAD)
            q_head = jnp.where(mine, q_pair, jnp.zeros_like(q_pair))
            scores = [nt_dot(k, q_head) for k in k_parts]
            top = jnp.max(scores[0], axis=0, keepdims=True)
            for s in scores[1:]:
                top = jnp.maximum(top, jnp.max(s, axis=0, keepdims=True))
            if not first:
                old_max = state_ref[max_row, :]
                top = jnp.maximum(top, old_max)
                shrink = jnp.exp2((old_max - top) * LOG2E)
            den, acc = 0.0, 0.0
            for s, v in zip(scores, v_parts):
                weights = jnp.exp2((s - top) * LOG2E)
                den = den + jnp.sum(weights, axis=0, keepdims=True)
                acc = acc + jnp.dot(
                    v[half * HEAD : (half + 1) * HEAD, :],
                    weights.astype(jnp.bfloat16),
                    preferred_element_type=jnp.float32,
                )
            if not first:
                den = den + state_ref[den_row, :] * shrink
                acc = acc + state_ref[rows, :] * shrink
            new_ref[max_row, :] = top
            new_ref[den_row, :] = den
            new_ref[rows, :] = acc


def fold(query_rows, blocks, state):
    row_count, features = query_rows.shape
    vmem = pl.BlockSpec(memory_space=pltpu.VMEM)
    operands = (query_rows, *blocks) if state is None else (query_rows, *blocks, state)
    key_count = sum(b.shape[0] for b in blocks)
    return pl.pallas_call(
        functools.partial(fold_kernel, state is None),
        out_shape=jax.ShapeDtypeStruct((features + 2 * STATS, row_count), jnp.float32),
        in_specs=[vmem] * len(operands),
        out_specs=vmem,
        compiler_params=pltpu.CompilerParams(vmem_limit_bytes=VMEM_LIMIT),
        cost_estimate=pl.CostEstimate(
            flops=4 * row_count * key_count * features,
            bytes_accessed=4 * key_count * features,
            transcendentals=row_count * key_count * (features // HEAD),
        ),
    )(*operands)


def merged(one_ref, two_ref, features):
    heads = features // HEAD
    max_rows, den_rows = (slice(features + i, features + i + heads) for i in (0, STATS))
    one_max, two_max = one_ref[max_rows, :], two_ref[max_rows, :]
    top = jnp.maximum(one_max, two_max)
    one, two = (jnp.exp2((m - top) * LOG2E) for m in (one_max, two_max))
    den = one_ref[den_rows, :] * one + two_ref[den_rows, :] * two
    one, two = one / den, two / den
    parts = []
    for head in range(heads):
        rows, row = slice(head * HEAD, (head + 1) * HEAD), slice(head, head + 1)
        parts.append(one_ref[rows, :] * one[row, :] + two_ref[rows, :] * two[row, :])
    return jnp.concatenate(parts, axis=0).astype(jnp.bfloat16).T


def project_kernel(depth, place_ref, one_ref, two_ref, self_ref, *refs):
    *got_refs, out_ref, attended, weight = refs
    z, core = place_ref[0], place_ref[1]
    rows, width = out_ref.shape
    features = attended.shape[1]
    pair = self_ref.shape[0]

    def put(chip, block):
        at = pl.multiple_of(lax.rem(chip, depth) * pair, 8)
        weight[pl.ds(at, pair), :] = block

    put(z, self_ref[...])
    step = 1
    for crossed, turned in zip(got_refs[::2], got_refs[1::2] + [None]):
        for here in range(0, crossed.shape[0], pair):
            block = slice(here, here + pair)
            ahead, behind = z + step, z + depth - step
            put(jnp.where(core == 0, behind, ahead), crossed[block, :])
            if turned is not None:
                put(jnp.where(core == 0, ahead, behind), turned[block, :])
            step += 1

    attended[...] = merged(one_ref, two_ref, features)
    mine = attended[pl.ds(pl.multiple_of(core * rows, 8), rows), :]
    chunk = width // 4
    for i in range(4):
        part = slice(i * chunk, (i + 1) * chunk)
        out_ref[:, part] = nt_dot(mine, weight[part, :]).astype(out_ref.dtype)


def project(depth, place, one, two, weights):
    row_count = one.shape[1]
    features = weights[0].shape[1]
    width = weights[0].shape[0] * depth
    vmem = pl.BlockSpec(memory_space=pltpu.VMEM)
    return pl.pallas_call(
        functools.partial(project_kernel, depth),
        out_shape=jax.ShapeDtypeStruct((row_count // 2, width), jnp.bfloat16),
        in_specs=[pl.BlockSpec(memory_space=pltpu.SMEM)] + [vmem] * (2 + len(weights)),
        out_specs=vmem,
        scratch_shapes=[
            pltpu.VMEM((row_count, features), jnp.bfloat16),
            pltpu.VMEM((width, features), jnp.bfloat16),
        ],
        compiler_params=pltpu.CompilerParams(vmem_limit_bytes=VMEM_LIMIT),
    )(place, one, two, *weights)


def weight_hops(depth):
    held, hops, last = 1, [], depth // 2
    while held <= last:
        hops.append(2 if held == 2 and last > 2 else 1)
        held += hops[-1]
    return hops


def on_device(query, keys, values, out_weight, out_gain):
    tokens, width = query.shape
    blk, uly = lax.axis_size("blk"), lax.axis_size("uly")
    depth = blk // 2
    last = depth // 2
    features = width // uly
    rows = tokens * uly
    at = lax.axis_index("blk").astype(jnp.int32)
    z, core = lax.div(at, 2), lax.rem(at, 2)
    swap = [(i, i ^ 1) for i in range(blk)]

    def round_z(hop):
        return [
            (2 * z + c, 2 * ((z + (hop if c == 0 else -hop)) % depth) + c)
            for z in range(depth)
            for c in range(2)
        ]

    ring = round_z(1)

    def by_core(own, other):
        return jnp.concatenate(
            [jnp.where(core == 0, own, other), jnp.where(core == 0, other, own)], axis=0
        )

    columns = out_weight.T
    w_self = by_core(columns, lax.ppermute(columns, "blk", swap))

    cut = [a.reshape(tokens, uly, features) for a in (query, keys, values)]
    packed = jnp.concatenate(cut, axis=2).transpose(1, 0, 2)
    own = lax.all_to_all(packed, "uly", 0, 0, tiled=True).reshape(rows, 3 * features)
    other = lax.ppermute(own, "blk", swap)
    q_all = by_core(own[:, :features], other[:, :features])
    q_all = q_all * jnp.bfloat16(1.0 / math.sqrt(HEAD))

    pair = w_self.shape[0]
    hops = weight_hops(depth)
    weights, held = [w_self], w_self
    for i, hop in enumerate(hops):
        crossing = [
            (2 * z + c, 2 * ((z + (-hop if c == 0 else hop)) % depth) + 1 - c)
            for z in range(depth)
            for c in range(2)
        ]
        weights.append(lax.ppermute(held[-hop * pair :], "blk", crossing))
        if i + 1 < len(hops):
            weights.append(lax.ppermute(weights[-1], "blk", swap))
            held = jnp.concatenate([held, weights[-1]], axis=0)[-2 * pair :]

    a, b = own[:, features:], other[:, features:]
    state = fold(q_all, (a,), None)
    for step in range(1, last + 1):
        a = lax.ppermute(a, "blk", ring)
        if step < last:
            b = lax.ppermute(b, "blk", ring)
        state = fold(q_all, (a, b) if step < last else (a,), state)
    theirs = lax.ppermute(state, "blk", swap)
    place = jnp.stack([z, core]).astype(jnp.int32)
    partial = project(depth, place, state, theirs, weights)
    blocks = lax.all_to_all(partial.reshape(uly, tokens, width), "uly", 0, 0, tiled=True)
    summed = jnp.sum(blocks.astype(jnp.float32), axis=0)
    return (out_gain * summed).astype(jnp.bfloat16)


def solution(mesh):
    in_specs = (
        P(("group", "blk", "uly"), None),
        P(("group", "blk", "uly"), None),
        P(("group", "blk", "uly"), None),
        P("uly", "blk"),
        P(),
    )
    out_specs = P(("group", "blk", "uly"), None)
    return jax.shard_map(
        on_device, mesh=mesh, in_specs=in_specs, out_specs=out_specs, check_vma=False
    )
```

```python
import functools
import math

import jax
import jax.numpy as jnp
from jax import lax
from jax.experimental import pallas as pl
from jax.experimental.pallas import tpu as pltpu
from jax.sharding import PartitionSpec as P


HEAD = 64
PAIR = 2 * HEAD
STATS = 8
VMEM_LIMIT = 16 * 1024 * 1024
STREAM_LIMIT = 60 * 1024 * 1024
LOG2E = math.log2(math.e)


def nt_dot(a, b):
    return lax.dot_general(a, b, (((1,), (1,)), ((), ())), preferred_element_type=jnp.float32)


def fold_head(q_head, k_parts, v_parts, old):
    scores = [nt_dot(k, q_head) for k in k_parts]
    top = jnp.max(scores[0], axis=0, keepdims=True)
    for s in scores[1:]:
        top = jnp.maximum(top, jnp.max(s, axis=0, keepdims=True))
    if old is not None:
        top = jnp.maximum(top, old[0])
    den, acc = 0.0, 0.0
    for s, v in zip(scores, v_parts):
        weights = jnp.exp2((s - top) * LOG2E)
        den = den + jnp.sum(weights, axis=0, keepdims=True)
        acc = acc + jnp.dot(v, weights.astype(jnp.bfloat16), preferred_element_type=jnp.float32)
    if old is not None:
        shrink = jnp.exp2((old[0] - top) * LOG2E)
        den = den + old[1] * shrink
        acc = acc + old[2] * shrink
    return top, den, acc


def rows_of(head, features):
    return (
        slice(features + head, features + head + 1),
        slice(features + STATS + head, features + STATS + head + 1),
        slice(head * HEAD, (head + 1) * HEAD),
    )


def head_of(q_pair, half):
    lane = lax.broadcasted_iota(jnp.int32, q_pair.shape, 1)
    mine = (lane < HEAD) if half == 0 else (lane >= HEAD)
    return jnp.where(mine, q_pair, jnp.zeros_like(q_pair))


def fold_kernel(first, q_ref, *refs):
    state_ref, new_ref = (None, refs[-1]) if first else refs[-2:]
    kv_refs = refs[:-1] if first else refs[:-2]
    features = q_ref.shape[1]
    for pair in range(features // PAIR):
        cols = slice(pair * PAIR, (pair + 1) * PAIR)
        q_pair = q_ref[:, cols]
        k_parts = [ref[:, cols] for ref in kv_refs]
        v_parts = [ref[:, slice(features + cols.start, features + cols.stop)].T for ref in kv_refs]
        for half in range(2):
            at = rows_of(2 * pair + half, features)
            old = None if first else tuple(state_ref[r, :] for r in at)
            v_half = [v[half * HEAD : (half + 1) * HEAD, :] for v in v_parts]
            for r, new in zip(at, fold_head(head_of(q_pair, half), k_parts, v_half, old)):
                new_ref[r, :] = new


def fold(query_rows, blocks, state):
    row_count, features = query_rows.shape
    vmem = pl.BlockSpec(memory_space=pltpu.VMEM)
    operands = (query_rows, *blocks) if state is None else (query_rows, *blocks, state)
    key_count = sum(b.shape[0] for b in blocks)
    return pl.pallas_call(
        functools.partial(fold_kernel, state is None),
        out_shape=jax.ShapeDtypeStruct((features + 2 * STATS, row_count), jnp.float32),
        in_specs=[vmem] * len(operands),
        out_specs=vmem,
        compiler_params=pltpu.CompilerParams(vmem_limit_bytes=VMEM_LIMIT),
        cost_estimate=pl.CostEstimate(
            flops=4 * row_count * key_count * features,
            bytes_accessed=4 * key_count * features,
            transcendentals=row_count * key_count * (features // HEAD),
        ),
    )(*operands)


def gathered_kernel(core_ref, q_ref, kv_ref, *refs):
    del core_ref
    weight_refs, (new_ref, weight_out) = refs[:-2], refs[-2:]
    keys = kv_ref.shape[2] // 2

    @pl.when(pl.program_id(0) == 0)
    def _():
        new_ref[: PAIR, :] = jnp.zeros_like(new_ref[: PAIR, :])
        new_ref[PAIR : PAIR + STATS, :] = jnp.full_like(new_ref[PAIR : PAIR + STATS, :], -jnp.inf)
        new_ref[PAIR + STATS :, :] = jnp.zeros_like(new_ref[PAIR + STATS :, :])

    q_pair = q_ref[...]
    k_parts = [kv_ref[i, 0, :keys, :] for i in range(kv_ref.shape[0])]
    v_parts = [kv_ref[i, 0, keys:, :].T for i in range(kv_ref.shape[0])]
    for half in range(2):
        at = rows_of(half, PAIR)
        old = tuple(new_ref[r, :] for r in at)
        v_half = [v[half * HEAD : (half + 1) * HEAD, :] for v in v_parts]
        for r, new in zip(at, fold_head(head_of(q_pair, half), k_parts, v_half, old)):
            new_ref[r, :] = new
    for i, ref in enumerate(weight_refs):
        weight_out[:, i * PAIR : (i + 1) * PAIR] = ref[...].reshape(-1, PAIR)


def fold_gathered(core, query_pair, gathered, keys, cols, features):
    row_count = query_pair.shape[0]
    blk = gathered.shape[0]
    depth = blk // 2
    steps = min(4, depth)
    chips = depth // steps
    by_chip = gathered.reshape(depth, 2, gathered.shape[1], PAIR)
    chunks = features // PAIR
    first = 2 * keys // cols
    weight_specs = [
        pl.BlockSpec((chips, 2, cols, PAIR), lambda i, core, at=first + f: (i, 0, at, 0))
        for f in range(chunks)
    ]
    return pl.pallas_call(
        gathered_kernel,
        out_shape=(
            jax.ShapeDtypeStruct((PAIR + 2 * STATS, row_count), jnp.float32),
            jax.ShapeDtypeStruct((blk * cols, features), jnp.bfloat16),
        ),
        grid_spec=pltpu.PrefetchScalarGridSpec(
            num_scalar_prefetch=1,
            grid=(steps,),
            in_specs=[
                pl.BlockSpec((row_count, PAIR), lambda i, core: (0, 0)),
                pl.BlockSpec((chips, 1, 2 * keys, PAIR), lambda i, core: (i, core[0], 0, 0)),
                *weight_specs,
            ],
            out_specs=(
                pl.BlockSpec((PAIR + 2 * STATS, row_count), lambda i, core: (0, 0)),
                pl.BlockSpec((2 * chips * cols, features), lambda i, core: (i, 0)),
            ),
        ),
        compiler_params=pltpu.CompilerParams(
            vmem_limit_bytes=STREAM_LIMIT, dimension_semantics=("arbitrary",)
        ),
        cost_estimate=pl.CostEstimate(
            flops=4 * row_count * depth * keys * PAIR,
            bytes_accessed=gathered.size * 2,
            transcendentals=row_count * depth * keys * 2,
        ),
    )(core[None], query_pair, by_chip, *[by_chip] * chunks)


def merged(one_ref, two_ref):
    features = one_ref.shape[0] - 2 * STATS
    heads = features // HEAD
    max_rows, den_rows = (slice(features + i, features + i + heads) for i in (0, STATS))
    one_max, two_max = one_ref[max_rows, :], two_ref[max_rows, :]
    top = jnp.maximum(one_max, two_max)
    one, two = (jnp.exp2((m - top) * LOG2E) for m in (one_max, two_max))
    den = one_ref[den_rows, :] * one + two_ref[den_rows, :] * two
    one, two = one / den, two / den
    parts = []
    for head in range(heads):
        rows, row = slice(head * HEAD, (head + 1) * HEAD), slice(head, head + 1)
        parts.append(one_ref[rows, :] * one[row, :] + two_ref[rows, :] * two[row, :])
    return jnp.concatenate(parts, axis=0).astype(jnp.bfloat16).T


def project_kernel(core_ref, one_ref, two_ref, pair_one_ref, pair_two_ref, weight_ref, out_ref, attended):
    rows, width = out_ref.shape
    ring = attended.shape[1] - PAIR
    attended[:, :ring] = merged(one_ref, two_ref)
    attended[:, ring:] = merged(pair_one_ref, pair_two_ref)
    mine = attended[pl.ds(pl.multiple_of(core_ref[0] * rows, 16), rows), :]
    chunk = width // 4
    for i in range(4):
        part = slice(i * chunk, (i + 1) * chunk)
        out_ref[:, part] = nt_dot(mine, weight_ref[part, :]).astype(out_ref.dtype)


def project(core, states, weight):
    row_count = states[0].shape[1]
    width, features = weight.shape
    vmem = pl.BlockSpec(memory_space=pltpu.VMEM)
    return pl.pallas_call(
        project_kernel,
        out_shape=jax.ShapeDtypeStruct((row_count // 2, width), jnp.bfloat16),
        in_specs=[pl.BlockSpec(memory_space=pltpu.SMEM)] + [vmem] * 5,
        out_specs=vmem,
        scratch_shapes=[pltpu.VMEM((row_count, features), jnp.bfloat16)],
        compiler_params=pltpu.CompilerParams(vmem_limit_bytes=VMEM_LIMIT),
    )(core[None], *states, weight)


def on_device(query, keys, values, out_weight, out_gain):
    tokens, width = query.shape
    blk, uly = lax.axis_size("blk"), lax.axis_size("uly")
    depth = blk // 2
    last = depth // 2
    features = width // uly
    ringed = features - PAIR
    rows = tokens * uly
    cols = out_weight.shape[1]
    core = (lax.axis_index("blk") % 2).astype(jnp.int32)
    swap = [(i, i ^ 1) for i in range(blk)]
    ring = [
        (2 * z + c, 2 * ((z + (1 if c == 0 else -1)) % depth) + c)
        for z in range(depth)
        for c in range(2)
    ]

    q, k, v = (a.reshape(tokens, uly, features) for a in (query, keys, values))
    pieces = (q, k[:, :, :ringed], v[:, :, :ringed], k[:, :, ringed:], v[:, :, ringed:])
    packed = jnp.concatenate(pieces, axis=2).transpose(1, 0, 2)
    own = lax.all_to_all(packed, "uly", 0, 0, tiled=True).reshape(rows, 3 * features)
    ends = (features, features + 2 * ringed, 3 * features - PAIR, 3 * features)

    columns = out_weight.T
    chunks = [columns[:, i : i + PAIR] for i in range(0, features, PAIR)]
    gathered = lax.all_gather(
        jnp.concatenate([own[:, ends[1] : ends[2]], own[:, ends[2] :], *chunks], axis=0), "blk"
    )
    other = lax.ppermute(own[:, : ends[1]], "blk", swap)
    q_own, q_other = own[:, :features], other[:, :features]
    q_all = jnp.concatenate(
        [jnp.where(core == 0, q_own, q_other), jnp.where(core == 0, q_other, q_own)], axis=0
    ) * jnp.bfloat16(1.0 / math.sqrt(HEAD))
    q_ring, q_pair = q_all[:, :ringed], q_all[:, ringed:]

    a, b = own[:, ends[0] : ends[1]], other[:, features:]
    state = fold(q_ring, (a,), None)
    for step in range(1, last + 1):
        a = lax.ppermute(a, "blk", ring)
        if step < last:
            b = lax.ppermute(b, "blk", ring)
        state = fold(q_ring, (a, b) if step < last else (a,), state)
    pair_state, weight = fold_gathered(core, q_pair, gathered, rows, cols, features)
    pair_theirs = lax.ppermute(pair_state, "blk", swap)
    theirs = lax.ppermute(state, "blk", swap)
    partial = project(core, (state, theirs, pair_state, pair_theirs), weight)
    blocks = lax.all_to_all(partial.reshape(uly, tokens, width), "uly", 0, 0, tiled=True)
    summed = jnp.sum(blocks.astype(jnp.float32), axis=0)
    return (out_gain * summed).astype(jnp.bfloat16)


def solution(mesh):
    in_specs = (
        P(("group", "blk", "uly"), None),
        P(("group", "blk", "uly"), None),
        P(("group", "blk", "uly"), None),
        P("uly", "blk"),
        P(),
    )
    out_specs = P(("group", "blk", "uly"), None)
    return jax.shard_map(
        on_device, mesh=mesh, in_specs=in_specs, out_specs=out_specs, check_vma=False
    )
```

```python
import functools
import math

import jax
import jax.numpy as jnp
from jax import lax
from jax.experimental import pallas as pl
from jax.experimental.pallas import tpu as pltpu
from jax.sharding import PartitionSpec as P


HEAD = 64
PAIR = 2 * HEAD
STATS = 8
VMEM_LIMIT = 16 * 1024 * 1024
LOG2E = math.log2(math.e)


def nt_dot(a, b):
    return lax.dot_general(a, b, (((1,), (1,)), ((), ())), preferred_element_type=jnp.float32)


def fold_kernel(first, q_ref, *refs):
    state_ref, new_ref = (None, refs[-1]) if first else refs[-2:]
    kv_refs = refs[:-1] if first else refs[:-2]
    features = q_ref.shape[1]
    for pair in range(features // PAIR):
        cols = slice(pair * PAIR, (pair + 1) * PAIR)
        q_pair = q_ref[:, cols]
        lane = lax.broadcasted_iota(jnp.int32, q_pair.shape, 1)
        k_parts = [ref[:, cols] for ref in kv_refs]
        v_parts = [ref[:, slice(features + cols.start, features + cols.stop)].T for ref in kv_refs]
        for half in range(2):
            head = 2 * pair + half
            rows = slice(head * HEAD, (head + 1) * HEAD)
            max_row = slice(features + head, features + head + 1)
            den_row = slice(features + STATS + head, features + STATS + head + 1)
            mine = (lane < HEAD) if half == 0 else (lane >= HEAD)
            q_head = jnp.where(mine, q_pair, jnp.zeros_like(q_pair))
            scores = [nt_dot(k, q_head) for k in k_parts]
            top = jnp.max(scores[0], axis=0, keepdims=True)
            for s in scores[1:]:
                top = jnp.maximum(top, jnp.max(s, axis=0, keepdims=True))
            if not first:
                old_max = state_ref[max_row, :]
                top = jnp.maximum(top, old_max)
                shrink = jnp.exp2((old_max - top) * LOG2E)
            den, acc = 0.0, 0.0
            for s, v in zip(scores, v_parts):
                weights = jnp.exp2((s - top) * LOG2E)
                den = den + jnp.sum(weights, axis=0, keepdims=True)
                acc = acc + jnp.dot(
                    v[half * HEAD : (half + 1) * HEAD, :],
                    weights.astype(jnp.bfloat16),
                    preferred_element_type=jnp.float32,
                )
            if not first:
                den = den + state_ref[den_row, :] * shrink
                acc = acc + state_ref[rows, :] * shrink
            new_ref[max_row, :] = top
            new_ref[den_row, :] = den
            new_ref[rows, :] = acc


def fold(query_rows, blocks, state):
    row_count, features = query_rows.shape
    vmem = pl.BlockSpec(memory_space=pltpu.VMEM)
    operands = (query_rows, *blocks) if state is None else (query_rows, *blocks, state)
    key_count = sum(b.shape[0] for b in blocks)
    return pl.pallas_call(
        functools.partial(fold_kernel, state is None),
        out_shape=jax.ShapeDtypeStruct((features + 2 * STATS, row_count), jnp.float32),
        in_specs=[vmem] * len(operands),
        out_specs=vmem,
        compiler_params=pltpu.CompilerParams(vmem_limit_bytes=VMEM_LIMIT),
        cost_estimate=pl.CostEstimate(
            flops=4 * row_count * key_count * features,
            bytes_accessed=4 * key_count * features,
            transcendentals=row_count * key_count * (features // HEAD),
        ),
    )(*operands)


def merged(one_ref, two_ref, features):
    heads = features // HEAD
    max_rows, den_rows = (slice(features + i, features + i + heads) for i in (0, STATS))
    one_max, two_max = one_ref[max_rows, :], two_ref[max_rows, :]
    top = jnp.maximum(one_max, two_max)
    one, two = (jnp.exp2((m - top) * LOG2E) for m in (one_max, two_max))
    den = one_ref[den_rows, :] * one + two_ref[den_rows, :] * two
    one, two = one / den, two / den
    parts = []
    for head in range(heads):
        rows, row = slice(head * HEAD, (head + 1) * HEAD), slice(head, head + 1)
        parts.append(one_ref[rows, :] * one[row, :] + two_ref[rows, :] * two[row, :])
    return jnp.concatenate(parts, axis=0).astype(jnp.bfloat16).T


def project_kernel(core_ref, one_ref, two_ref, weight_ref, out_ref, attended):
    rows, width = out_ref.shape
    attended[...] = merged(one_ref, two_ref, attended.shape[1])
    mine = attended[pl.ds(pl.multiple_of(core_ref[0] * rows, 16), rows), :]
    chunk = width // 4
    for i in range(4):
        part = slice(i * chunk, (i + 1) * chunk)
        out_ref[:, part] = nt_dot(mine, weight_ref[part, :]).astype(out_ref.dtype)


def project(core, one, two, weight):
    row_count = one.shape[1]
    width, features = weight.shape
    vmem = pl.BlockSpec(memory_space=pltpu.VMEM)
    return pl.pallas_call(
        project_kernel,
        out_shape=jax.ShapeDtypeStruct((row_count // 2, width), jnp.bfloat16),
        in_specs=[pl.BlockSpec(memory_space=pltpu.SMEM)] + [vmem] * 3,
        out_specs=vmem,
        scratch_shapes=[pltpu.VMEM((row_count, features), jnp.bfloat16)],
        compiler_params=pltpu.CompilerParams(vmem_limit_bytes=VMEM_LIMIT),
    )(core[None], one, two, weight)


def on_device(query, keys, values, out_weight, out_gain):
    tokens, width = query.shape
    blk, uly = lax.axis_size("blk"), lax.axis_size("uly")
    depth = blk // 2
    last = depth // 2
    features = width // uly
    rows = tokens * uly
    core = lax.rem(lax.axis_index("blk").astype(jnp.int32), 2)
    swap = [(i, i ^ 1) for i in range(blk)]
    ring = [
        (2 * z + c, 2 * ((z + (1 if c == 0 else -1)) % depth) + c)
        for z in range(depth)
        for c in range(2)
    ]

    def by_core(own, other):
        return jnp.concatenate(
            [jnp.where(core == 0, own, other), jnp.where(core == 0, other, own)], axis=0
        )

    weight = lax.all_gather(out_weight, "blk", axis=1, tiled=True).T

    cut = [a.reshape(tokens, uly, features) for a in (query, keys, values)]
    packed = jnp.concatenate(cut, axis=2).transpose(1, 0, 2)
    own = lax.all_to_all(packed, "uly", 0, 0, tiled=True).reshape(rows, 3 * features)
    other = lax.ppermute(own, "blk", swap)
    q_all = by_core(own[:, :features], other[:, :features])
    q_all = q_all * jnp.bfloat16(1.0 / math.sqrt(HEAD))

    a, b = own[:, features:], other[:, features:]
    state = fold(q_all, (a,), None)
    for step in range(1, last + 1):
        a = lax.ppermute(a, "blk", ring)
        if step < last:
            b = lax.ppermute(b, "blk", ring)
        state = fold(q_all, (a, b) if step < last else (a,), state)
    theirs = lax.ppermute(state, "blk", swap)
    partial = project(core, state, theirs, weight)
    blocks = lax.all_to_all(partial.reshape(uly, tokens, width), "uly", 0, 0, tiled=True)
    summed = jnp.sum(blocks.astype(jnp.float32), axis=0)
    return (out_gain * summed).astype(jnp.bfloat16)


def solution(mesh):
    in_specs = (
        P(("group", "blk", "uly"), None),
        P(("group", "blk", "uly"), None),
        P(("group", "blk", "uly"), None),
        P("uly", "blk"),
        P(),
    )
    out_specs = P(("group", "blk", "uly"), None)
    return jax.shard_map(
        on_device, mesh=mesh, in_specs=in_specs, out_specs=out_specs, check_vma=False
    )
```

```python
import functools
import math

import jax
import jax.numpy as jnp
from jax import lax
from jax.experimental import pallas as pl
from jax.experimental.pallas import tpu as pltpu
from jax.sharding import PartitionSpec as P


HEAD = 64
PAIR = 2 * HEAD
STATS = 8
VMEM_LIMIT = 16 * 1024 * 1024
ALL_VMEM = 67043328
LOG2E = math.log2(math.e)


def nt_dot(a, b):
    return lax.dot_general(a, b, (((1,), (1,)), ((), ())), preferred_element_type=jnp.float32)


def fold_kernel(first, q_ref, *refs):
    state_ref, new_ref = (None, refs[-1]) if first else refs[-2:]
    kv_refs = refs[:-1] if first else refs[:-2]
    features = q_ref.shape[1]
    for pair in range(features // PAIR):
        cols = slice(pair * PAIR, (pair + 1) * PAIR)
        q_pair = q_ref[:, cols]
        lane = lax.broadcasted_iota(jnp.int32, q_pair.shape, 1)
        k_parts = [ref[:, cols] for ref in kv_refs]
        v_parts = [ref[:, slice(features + cols.start, features + cols.stop)].T for ref in kv_refs]
        for half in range(2):
            head = 2 * pair + half
            rows = slice(head * HEAD, (head + 1) * HEAD)
            max_row = slice(features + head, features + head + 1)
            den_row = slice(features + STATS + head, features + STATS + head + 1)
            mine = (lane < HEAD) if half == 0 else (lane >= HEAD)
            q_head = jnp.where(mine, q_pair, jnp.zeros_like(q_pair))
            scores = [nt_dot(k, q_head) for k in k_parts]
            top = jnp.max(scores[0], axis=0, keepdims=True)
            for s in scores[1:]:
                top = jnp.maximum(top, jnp.max(s, axis=0, keepdims=True))
            if not first:
                old_max = state_ref[max_row, :]
                top = jnp.maximum(top, old_max)
                shrink = jnp.exp2((old_max - top) * LOG2E)
            den, acc = 0.0, 0.0
            for s, v in zip(scores, v_parts):
                weights = jnp.exp2((s - top) * LOG2E)
                den = den + jnp.sum(weights, axis=0, keepdims=True)
                acc = acc + jnp.dot(
                    v[half * HEAD : (half + 1) * HEAD, :],
                    weights.astype(jnp.bfloat16),
                    preferred_element_type=jnp.float32,
                )
            if not first:
                den = den + state_ref[den_row, :] * shrink
                acc = acc + state_ref[rows, :] * shrink
            new_ref[max_row, :] = top
            new_ref[den_row, :] = den
            new_ref[rows, :] = acc


def fold(query_rows, blocks, state):
    row_count, features = query_rows.shape
    vmem = pl.BlockSpec(memory_space=pltpu.VMEM)
    operands = (query_rows, *blocks) if state is None else (query_rows, *blocks, state)
    key_count = sum(b.shape[0] for b in blocks)
    return pl.pallas_call(
        functools.partial(fold_kernel, state is None),
        out_shape=jax.ShapeDtypeStruct((features + 2 * STATS, row_count), jnp.float32),
        in_specs=[vmem] * len(operands),
        out_specs=vmem,
        compiler_params=pltpu.CompilerParams(vmem_limit_bytes=VMEM_LIMIT),
        cost_estimate=pl.CostEstimate(
            flops=4 * row_count * key_count * features,
            bytes_accessed=4 * key_count * features,
            transcendentals=row_count * key_count * (features // HEAD),
        ),
    )(*operands)


def merged(one_ref, two_ref, features):
    heads = features // HEAD
    max_rows, den_rows = (slice(features + i, features + i + heads) for i in (0, STATS))
    one_max, two_max = one_ref[max_rows, :], two_ref[max_rows, :]
    top = jnp.maximum(one_max, two_max)
    one, two = (jnp.exp2((m - top) * LOG2E) for m in (one_max, two_max))
    den = one_ref[den_rows, :] * one + two_ref[den_rows, :] * two
    one, two = one / den, two / den
    parts = []
    for head in range(heads):
        rows, row = slice(head * HEAD, (head + 1) * HEAD), slice(head, head + 1)
        parts.append(one_ref[rows, :] * one[row, :] + two_ref[rows, :] * two[row, :])
    return jnp.concatenate(parts, axis=0).astype(jnp.bfloat16).T


def project_kernel(core_ref, one_ref, two_ref, weight_ref, out_ref, attended):
    rows, width = out_ref.shape
    attended[...] = merged(one_ref, two_ref, attended.shape[1])
    mine = attended[pl.ds(pl.multiple_of(core_ref[0] * rows, 16), rows), :]
    chunk = width // 4
    for i in range(4):
        part = slice(i * chunk, (i + 1) * chunk)
        out_ref[:, part] = nt_dot(mine, weight_ref[part, :]).astype(out_ref.dtype)


def project(core, one, two, weight):
    row_count = one.shape[1]
    width, features = weight.shape
    vmem = pl.BlockSpec(memory_space=pltpu.VMEM)
    return pl.pallas_call(
        project_kernel,
        out_shape=jax.ShapeDtypeStruct((row_count // 2, width), jnp.bfloat16),
        in_specs=[pl.BlockSpec(memory_space=pltpu.SMEM)] + [vmem] * 3,
        out_specs=vmem,
        scratch_shapes=[pltpu.VMEM((row_count, features), jnp.bfloat16)],
        compiler_params=pltpu.CompilerParams(vmem_limit_bytes=VMEM_LIMIT),
    )(core[None], one, two, weight)


def pack_kernel(*refs):
    count = (len(refs) - 2) // 2
    in_refs, out_ref, held_refs, sems = refs[:count], refs[count], refs[count + 1 : -1], refs[-1]
    features = out_ref.shape[2] // count
    copies = [
        pltpu.make_async_copy(ref, held, sems.at[i])
        for i, (ref, held) in enumerate(zip(in_refs, held_refs))
    ]
    for copy in copies:
        copy.start()
    for i, (copy, held) in enumerate(zip(copies, held_refs)):
        copy.wait()
        for to in range(out_ref.shape[0]):
            out_ref[to, :, i * features : (i + 1) * features] = held[
                :, to * features : (to + 1) * features
            ]


def pack(arrays, parts):
    tokens, width = arrays[0].shape
    count = len(arrays)
    return pl.pallas_call(
        pack_kernel,
        out_shape=jax.ShapeDtypeStruct((parts, tokens, count * (width // parts)), arrays[0].dtype),
        in_specs=[pl.BlockSpec(memory_space=pltpu.HBM)] * count,
        out_specs=pl.BlockSpec(memory_space=pltpu.VMEM),
        scratch_shapes=[pltpu.VMEM(a.shape, a.dtype) for a in arrays]
        + [pltpu.SemaphoreType.DMA((count,))],
        compiler_params=pltpu.CompilerParams(vmem_limit_bytes=ALL_VMEM),
    )(*arrays)


def on_device(query, keys, values, out_weight, out_gain):
    tokens, width = query.shape
    blk, uly = lax.axis_size("blk"), lax.axis_size("uly")
    depth = blk // 2
    last = depth // 2
    features = width // uly
    rows = tokens * uly
    core = lax.rem(lax.axis_index("blk").astype(jnp.int32), 2)
    swap = [(i, i ^ 1) for i in range(blk)]
    ring = [
        (2 * z + c, 2 * ((z + (1 if c == 0 else -1)) % depth) + c)
        for z in range(depth)
        for c in range(2)
    ]

    def by_core(own, other):
        return jnp.concatenate(
            [jnp.where(core == 0, own, other), jnp.where(core == 0, other, own)], axis=0
        )

    weight = lax.all_gather(out_weight, "blk", axis=1, tiled=True).T

    packed = pack((query, keys, values), uly)
    own = lax.all_to_all(packed, "uly", 0, 0, tiled=True).reshape(rows, 3 * features)
    other = lax.ppermute(own, "blk", swap)
    q_all = by_core(own[:, :features], other[:, :features])
    q_all = q_all * jnp.bfloat16(1.0 / math.sqrt(HEAD))

    a, b = own[:, features:], other[:, features:]
    state = fold(q_all, (a,), None)
    for step in range(1, last + 1):
        a = lax.ppermute(a, "blk", ring)
        if step < last:
            b = lax.ppermute(b, "blk", ring)
        state = fold(q_all, (a, b) if step < last else (a,), state)
    theirs = lax.ppermute(state, "blk", swap)
    partial = project(core, state, theirs, weight)
    blocks = lax.all_to_all(partial.reshape(uly, tokens, width), "uly", 0, 0, tiled=True)
    summed = jnp.sum(blocks.astype(jnp.float32), axis=0)
    return (out_gain * summed).astype(jnp.bfloat16)


def solution(mesh):
    in_specs = (
        P(("group", "blk", "uly"), None),
        P(("group", "blk", "uly"), None),
        P(("group", "blk", "uly"), None),
        P("uly", "blk"),
        P(),
    )
    out_specs = P(("group", "blk", "uly"), None)
    return jax.shard_map(
        on_device, mesh=mesh, in_specs=in_specs, out_specs=out_specs, check_vma=False
    )
```
